32 devices in a mesh: samp: 16 (over z, y, x), tgt: 2 (over core).
Axes of the slice: x: 2, y: 2, z: 4, core: 2. Of those that a mesh axis runs over, the one named last changes fastest.
Arguments:
- samples: bfloat16 [3072, 128], P('samp'), may hold values from -6 to 6
- omega: bfloat16 [128, 4096], replicated, may hold values from -0.5 to 0.5
- phase: float32 [4096], replicated, may hold values from -3.140625 to 3.140625
- right_side: float32 [4096, 512], P('samp', 'tgt'), may hold values from -6 to 6
Outputs:
- weights: float32 [4096, 512], P('samp', 'tgt')
The draws below stay inside these ranges and needn't reach their ends.
All inputs are finite; a program needn't handle non-finite values.
Results may differ from the reference program's by a relative error of at most 0.011.
The reference program's roundings to bfloat16 on the way count: a program that leaves them out, or rounds other values in their place, can miss the bound.
Values may be sent and summed in bfloat16 or wider, within the bound.
No kernel may reach another device: no remote copies, remote signals or barrier semaphores. Data moves between devices by JAX's collectives and lax.ppermute only.
A program may use at most 128 MiB of HBM per device.

```python
import jax
import jax.numpy as jnp
from jax import lax

F = 4096
K = 512
DX = 128
ITERS = 2
N = 3072


def steps_of(rng, shape, shards, least, top_value):
    factor_of = 1.0
    for dim, blocks in shards:
        heights = jax.random.uniform(jax.random.fold_in(jax.random.fold_in(rng, 6), dim), (blocks,), jnp.float32, least / len(shards), top_value / len(shards))
        factor_of = factor_of * jnp.repeat(jnp.exp(heights), shape[dim] // blocks).reshape((-1,) + (1,) * (len(shape) - 1 - dim))
    return factor_of


def gaussian(rng, shape, deviation, bound, shards=(), held_as=jnp.bfloat16):
    values = jax.random.normal(rng, shape, jnp.float32) * deviation
    if len(shards) > 0:
        values = steps_of(rng, shape, shards, -0.22, 0.18) * values
    return jnp.clip(values, min=-bound, max=bound).astype(held_as)


def setup_inputs(seed: int = 0) -> dict:
    streams_of = jax.random.split(jax.random.key(seed), 5)
    return {
        "samples": gaussian(streams_of[0], (N, DX), 1.0, 6.0, ((0, 16),)),
        "omega": gaussian(streams_of[1], (DX, F), DX ** -0.5, 0.5),
        "phase": jnp.clip(jax.random.uniform(streams_of[2], (F,), jnp.float32, -3.140625, 3.140625), -3.140625, 3.140625),
        "right_side": gaussian(streams_of[3], (F, K), 1.0, 6.0, ((0, 16), (1, 2)), jnp.float32),
    }


ridge = 1.0

def precise_dot(left_matrix, right_matrix):
    return jnp.dot(left_matrix, right_matrix, precision=lax.Precision.HIGHEST)

def spd_solve(gram_matrix, rhs_matrix):
    factor = jnp.linalg.cholesky(gram_matrix)
    return jax.scipy.linalg.cho_solve((factor, True), rhs_matrix)

def reference(samples, omega, phase, right_side):
    preact = jnp.dot(samples.astype(jnp.float32), omega.astype(jnp.float32), preferred_element_type=jnp.float32) + phase
    features = jnp.cos(preact).astype(jnp.bfloat16)
    sample_total = features.shape[0]
    weights = jnp.zeros_like(right_side)
    residual = right_side
    direction = right_side
    gram_rr = precise_dot(residual.T, residual)
    for iteration in range(ITERS):
        projected = jnp.dot(features.astype(jnp.float32), direction.astype(jnp.bfloat16).astype(jnp.float32), preferred_element_type=jnp.float32).astype(jnp.bfloat16)
        image = jnp.dot(features.T.astype(jnp.float32), projected.astype(jnp.float32), preferred_element_type=jnp.float32) / sample_total + ridge * direction
        alpha_coef = spd_solve(precise_dot(direction.T, image), gram_rr)
        weights = weights + precise_dot(direction, alpha_coef)
        residual = residual - precise_dot(image, alpha_coef)
        gram_new = precise_dot(residual.T, residual)
        beta_coef = spd_solve(gram_rr, gram_new)
        direction = residual + precise_dot(direction, beta_coef)
        gram_rr = gram_new
    return weights
```

```python
import functools

import jax
import jax.numpy as jnp
from jax import lax
from jax.experimental import pallas as pl
from jax.experimental.pallas import tpu as pltpu
from jax.sharding import PartitionSpec as P

ITERS = 2
PIVOTS = 4
LANES = 128

ridge = 1.0


def precise_dot(left_matrix, right_matrix):
    return jnp.dot(left_matrix, right_matrix, precision=lax.Precision.HIGHEST)


def tile_inverse(tile):
    size = tile.shape[0]
    lane = lax.broadcasted_iota(jnp.int32, (1, size), 1)
    sub = lax.broadcasted_iota(jnp.int32, (8, size), 0)

    def group(_, mat):
        for first in range(0, 8, PIVOTS):
            spots = list(range(first, first + PIVOTS))
            cols = [jnp.broadcast_to(mat[:, j : j + 1], (size, size)) for j in spots]
            pivot_lanes = (lane >= first) & (lane < first + PIVOTS)
            rows = [
                jnp.where(pivot_lanes, jnp.where(lane == j, 1.0, 0.0), mat[j : j + 1, :]) for j in spots
            ]
            small = [[cols[b][spots[a] : spots[a] + 1, :] for b in range(PIVOTS)] for a in range(PIVOTS)]
            for a in range(PIVOTS):
                scale = 1.0 / small[a][a]
                rows[a] = rows[a] * scale
                small[a] = [v * scale for v in small[a]]
                for c in range(PIVOTS):
                    if c != a:
                        factor = small[c][a]
                        rows[c] = rows[c] - factor * rows[a]
                        small[c] = [
                            small[c][b] - factor * small[a][b] if b > a else small[c][b]
                            for b in range(PIVOTS)
                        ]
            mat = jnp.where(pivot_lanes, 0.0, mat)
            for a in range(PIVOTS):
                mat = mat - cols[a] * rows[a]
            top = mat[:8]
            for a, j in enumerate(spots):
                top = jnp.where(sub == j, rows[a], top)
            mat = jnp.concatenate([top, mat[8:]], axis=0)
        mat = jnp.concatenate([mat[8:], mat[:8]], axis=0)
        return pltpu.roll(mat, size - 8, 1)

    return lax.fori_loop(0, size // 8, group, tile)


def inverse_kernel(gram_ref, out_ref):
    size = gram_ref.shape[0]
    dot = functools.partial(
        jnp.dot, precision=lax.Precision.HIGHEST, preferred_element_type=jnp.float32
    )
    out_ref[...] = gram_ref[...]

    def step(begin):
        inv = tile_inverse(out_ref[pl.ds(begin, LANES), pl.ds(begin, LANES)])
        panel = out_ref[:, pl.ds(begin, LANES)]
        new_rows = dot(inv, out_ref[pl.ds(begin, LANES), :])
        out_ref[...] = out_ref[...] - dot(panel, new_rows)
        out_ref[:, pl.ds(begin, LANES)] = -dot(panel, inv)
        out_ref[pl.ds(begin, LANES), :] = new_rows
        out_ref[pl.ds(begin, LANES), pl.ds(begin, LANES)] = inv

    for begin in range(0, size, LANES):
        step(begin)


def spd_inverse(gram_matrix):
    return pl.pallas_call(
        inverse_kernel,
        out_shape=jax.ShapeDtypeStruct(gram_matrix.shape, jnp.float32),
        name="spd_inverse",
    )(gram_matrix)


def cosine_features(samples, omega, phase):
    preact = jnp.dot(samples, omega, preferred_element_type=jnp.float32) + phase
    return jnp.cos(preact).astype(jnp.bfloat16)


def gram(left, right):
    return lax.dot_general(
        left, right, (((0,), (0,)), ((), ())), preferred_element_type=jnp.float32
    )


def wide_dot(narrow, wide):
    high = wide.astype(jnp.bfloat16)
    low = (wide - high.astype(jnp.float32)).astype(jnp.bfloat16)
    return jnp.dot(narrow, high, preferred_element_type=jnp.float32) + jnp.dot(
        narrow, low, preferred_element_type=jnp.float32
    )


def body(samples, omega, phase, right_side):
    feat_rows, col_count = right_side.shape
    sample_total = samples.shape[0] * lax.axis_size("samp")
    col_offset = lax.axis_index("tgt") * col_count
    row_offset = lax.axis_index("samp") * feat_rows

    def own_columns(whole):
        return lax.dynamic_slice_in_dim(whole, col_offset, col_count, 1)

    def gather_rows(piece):
        return lax.all_gather(piece, "samp", axis=0, tiled=True)

    def gather_columns(piece):
        return lax.all_gather(piece, "tgt", axis=1, tiled=True)

    start_half = gather_rows(right_side.astype(jnp.bfloat16))
    all_samples = gather_rows(samples)
    start_rows = gather_columns(right_side)
    feats_own = cosine_features(samples, omega, phase)
    feats_cols = cosine_features(
        all_samples,
        lax.dynamic_slice_in_dim(omega, row_offset, feat_rows, 1),
        lax.dynamic_slice_in_dim(phase, row_offset, feat_rows, 0),
    )

    def project(direction_half):
        own = jnp.dot(feats_own, direction_half, preferred_element_type=jnp.float32)
        return gather_columns(gather_rows(own.astype(jnp.bfloat16)))

    proj = project(start_half)
    start = gather_columns(start_half)
    gram_rr = gram(start, start)
    inv_rr = spd_inverse(gram_rr)
    gram_pq = ridge * gram_rr + gram(proj, proj) / sample_total
    alpha = precise_dot(spd_inverse(gram_pq), gram_rr)
    image_rows = gram(feats_cols, proj) / sample_total + ridge * start_rows
    resid_rows = start_rows - precise_dot(image_rows, alpha)
    resid = gather_columns(gather_rows(own_columns(resid_rows).astype(jnp.bfloat16)))
    gram_new = gram(resid, resid)
    beta = precise_dot(inv_rr, gram_new)
    direction = (resid.astype(jnp.float32) + wide_dot(start, beta)).astype(jnp.bfloat16)
    proj_next = project(own_columns(direction))
    direction_rows = resid_rows + precise_dot(start_rows, beta)
    gram_next = ridge * gram(direction, direction) + gram(proj_next, proj_next) / sample_total
    alpha_next = precise_dot(spd_inverse(gram_next), own_columns(gram_new))
    return precise_dot(start_rows, own_columns(alpha)) + precise_dot(direction_rows, alpha_next)


def solution(mesh):
    placed = (P("samp", None), P(), P(), P("samp", "tgt"))
    return jax.shard_map(
        body, mesh=mesh, in_specs=placed, out_specs=P("samp", "tgt"), check_vma=False
    )
```

```python
import functools

import jax
import jax.numpy as jnp
from jax import lax
from jax.experimental import pallas as pl
from jax.experimental.pallas import tpu as pltpu
from jax.sharding import PartitionSpec as P

ITERS = 2
PIVOTS = 4
LANES = 128

ridge = 1.0


def precise_dot(left_matrix, right_matrix):
    return jnp.dot(left_matrix, right_matrix, precision=lax.Precision.HIGHEST)


def tile_inverse(tile):
    size = tile.shape[0]
    lane = lax.broadcasted_iota(jnp.int32, (1, size), 1)
    sub = lax.broadcasted_iota(jnp.int32, (8, size), 0)

    def group(_, mat):
        for first in range(0, 8, PIVOTS):
            spots = list(range(first, first + PIVOTS))
            cols = [jnp.broadcast_to(mat[:, j : j + 1], (size, size)) for j in spots]
            pivot_lanes = (lane >= first) & (lane < first + PIVOTS)
            rows = [
                jnp.where(pivot_lanes, jnp.where(lane == j, 1.0, 0.0), mat[j : j + 1, :]) for j in spots
            ]
            small = [[cols[b][spots[a] : spots[a] + 1, :] for b in range(PIVOTS)] for a in range(PIVOTS)]
            for a in range(PIVOTS):
                scale = 1.0 / small[a][a]
                rows[a] = rows[a] * scale
                small[a] = [v * scale for v in small[a]]
                for c in range(PIVOTS):
                    if c != a:
                        factor = small[c][a]
                        rows[c] = rows[c] - factor * rows[a]
                        small[c] = [
                            small[c][b] - factor * small[a][b] if b > a else small[c][b]
                            for b in range(PIVOTS)
                        ]
            mat = jnp.where(pivot_lanes, 0.0, mat)
            for a in range(PIVOTS):
                mat = mat - cols[a] * rows[a]
            top = mat[:8]
            for a, j in enumerate(spots):
                top = jnp.where(sub == j, rows[a], top)
            mat = jnp.concatenate([top, mat[8:]], axis=0)
        mat = jnp.concatenate([mat[8:], mat[:8]], axis=0)
        return pltpu.roll(mat, size - 8, 1)

    return lax.fori_loop(0, size // 8, group, tile)


def inverse_kernel(gram_ref, out_ref):
    size = gram_ref.shape[0]
    dot = functools.partial(
        jnp.dot, precision=lax.Precision.HIGHEST, preferred_element_type=jnp.float32
    )
    out_ref[...] = gram_ref[...]

    def step(begin):
        inv = tile_inverse(out_ref[pl.ds(begin, LANES), pl.ds(begin, LANES)])
        panel = out_ref[:, pl.ds(begin, LANES)]
        new_rows = dot(inv, out_ref[pl.ds(begin, LANES), :])
        out_ref[...] = out_ref[...] - dot(panel, new_rows)
        out_ref[:, pl.ds(begin, LANES)] = -dot(panel, inv)
        out_ref[pl.ds(begin, LANES), :] = new_rows
        out_ref[pl.ds(begin, LANES), pl.ds(begin, LANES)] = inv

    for begin in range(0, size, LANES):
        step(begin)


def spd_inverse(gram_matrix):
    return pl.pallas_call(
        inverse_kernel,
        out_shape=jax.ShapeDtypeStruct(gram_matrix.shape, jnp.float32),
        name="spd_inverse",
    )(gram_matrix)


def cosine_features(samples, omega, phase):
    preact = jnp.dot(samples, omega, preferred_element_type=jnp.float32) + phase
    return jnp.cos(preact).astype(jnp.bfloat16)


def gram(left, right):
    return lax.dot_general(
        left, right, (((0,), (0,)), ((), ())), preferred_element_type=jnp.float32
    )


def wide_dot(narrow, wide):
    high = wide.astype(jnp.bfloat16)
    low = (wide - high.astype(jnp.float32)).astype(jnp.bfloat16)
    return jnp.dot(narrow, high, preferred_element_type=jnp.float32) + jnp.dot(
        narrow, low, preferred_element_type=jnp.float32
    )


def body(samples, omega, phase, right_side):
    feat_rows, col_count = right_side.shape
    sample_total = samples.shape[0] * lax.axis_size("samp")
    col_offset = lax.axis_index("tgt") * col_count
    row_offset = lax.axis_index("samp") * feat_rows

    def own_columns(whole):
        return lax.dynamic_slice_in_dim(whole, col_offset, col_count, 1)

    def gather_rows(piece):
        return lax.all_gather(piece, "samp", axis=0, tiled=True)

    def gather_columns(piece):
        return lax.all_gather(piece, "tgt", axis=1, tiled=True)

    packed = jnp.concatenate(
        [right_side.astype(jnp.bfloat16), samples.reshape(-1, col_count)], axis=0
    )
    packed = gather_rows(packed[None])
    start_half = packed[:, :feat_rows].reshape(-1, col_count)
    all_samples = packed[:, feat_rows:].reshape(-1, samples.shape[1])
    start = gather_columns(start_half)
    gram_rr = gram(start, start)
    inv_rr = spd_inverse(gram_rr)
    start_rows = gather_columns(right_side)
    feats_own = cosine_features(samples, omega, phase)
    feats_cols = cosine_features(
        all_samples,
        lax.dynamic_slice_in_dim(omega, row_offset, feat_rows, 1),
        lax.dynamic_slice_in_dim(phase, row_offset, feat_rows, 0),
    )

    def project(direction_half):
        own = jnp.dot(feats_own, direction_half, preferred_element_type=jnp.float32)
        return gather_rows(own.astype(jnp.bfloat16))

    proj_half, inv_rr, feats_cols = lax.optimization_barrier((project(start_half), inv_rr, feats_cols))
    proj = gather_columns(proj_half)
    gram_pq = ridge * gram_rr + gram(proj, proj) / sample_total
    alpha = precise_dot(spd_inverse(gram_pq), gram_rr)
    image_rows = gram(feats_cols, proj) / sample_total + ridge * start_rows
    resid_rows = start_rows - precise_dot(image_rows, alpha)
    resid = gather_columns(gather_rows(own_columns(resid_rows).astype(jnp.bfloat16)))
    gram_new = gram(resid, resid)
    beta = precise_dot(inv_rr, gram_new)
    direction = (resid.astype(jnp.float32) + wide_dot(start, beta)).astype(jnp.bfloat16)
    proj_next = gather_columns(project(own_columns(direction)))
    direction_rows = resid_rows + precise_dot(start_rows, beta)
    gram_next = ridge * gram(direction, direction) + gram(proj_next, proj_next) / sample_total
    alpha_next = precise_dot(spd_inverse(gram_next), own_columns(gram_new))
    return precise_dot(start_rows, own_columns(alpha)) + precise_dot(direction_rows, alpha_next)


def solution(mesh):
    placed = (P("samp", None), P(), P(), P("samp", "tgt"))
    return jax.shard_map(
        body, mesh=mesh, in_specs=placed, out_specs=P("samp", "tgt"), check_vma=False
    )
```
